256 devices in a mesh: par: 16 (over x, z_hi, core), freq: 16 (over z_lo, y).
Axes of the slice: x: 4, y: 4, z: 8 (z_hi: 2, z_lo: 4; z = z_hi * 4 + z_lo), core: 2. Of those that a mesh axis runs over, the one named last changes fastest.
Arguments:
- probes: bfloat16 [64, 600, 420], P('freq'), may hold values from -6 to 6
- map_real: bfloat16 [224, 600, 4096], P('freq', None, 'par'), may hold values from -0.09375 to 0.09375
- map_imag: bfloat16 [224, 600, 4096], P('freq', None, 'par'), may hold values from -0.09375 to 0.09375
- prior_var: float32 [4096], P('par'), may hold values from 0.05 to 13, as said below
Outputs:
- applied: bfloat16 [64, 600, 420], P('freq')
The draws below stay inside these ranges and needn't reach their ends.
Inputs may be any that keep to these rules, and one draw needn't show every extreme that they name: `prior_var`: prior variances are positive.
All inputs are finite; a program needn't handle non-finite values.
Results may differ from the reference program's by a relative error of at most 0.014.
Values may be sent and summed in bfloat16 or wider, within the bound.
No kernel may reach another device: no remote copies, remote signals or barrier semaphores. Data moves between devices by JAX's collectives and lax.ppermute only.
A program may use at most 64 MiB of HBM per device.

```python
import jax
import jax.numpy as jnp
from jax import lax

SENSORS = 600
STEPS = 420
PERIOD = 840
PARAMS = 4096
BINS = 224
PROBES = 64


def draw_prior_var(key, part):
    position = jnp.arange(PARAMS, dtype=jnp.float32) / PARAMS
    ramp = jnp.exp(jnp.log(8.0) * position) / 3.0
    rough = jnp.exp(jax.random.uniform(key, (PARAMS,), jnp.float32, jnp.log(0.5), jnp.log(2.0)))
    return (ramp * rough).astype(jnp.float32)


def block_scale(stream_key, extent, split, low, top_value):
    loudness, own = 1.0, jax.random.fold_in(stream_key, 6)
    for axis_at, blocks in split:
        draws = jnp.exp(jax.random.uniform(jax.random.fold_in(own, axis_at), (blocks,), jnp.float32, low / len(split), top_value / len(split)))
        loudness = loudness * jnp.repeat(draws, extent[axis_at] // blocks).reshape([-1 if axis == axis_at else 1 for axis in range(len(extent))])
    return loudness


def bell_draw(key, dims, width, reach, pieces=(), kind=jnp.bfloat16):
    gain = block_scale(key, dims, pieces, -0.22, 0.18) if pieces else 1.0
    values = jax.random.normal(key, dims, jnp.float32) * width * gain
    return jnp.minimum(jnp.maximum(values, -reach), reach).astype(kind)


def setup_inputs(seed: int = 0) -> dict:
    key_list = jax.random.split(jax.random.key(seed), 5)
    probes = bell_draw(key_list[0], (PROBES, SENSORS, STEPS), 1.0, 6.0, ((0, 16),))
    map_real = bell_draw(key_list[1], (BINS, SENSORS, PARAMS), PARAMS ** -0.5, 0.09375, ((0, 16), (2, 16)))
    map_imag = bell_draw(key_list[2], (BINS, SENSORS, PARAMS), PARAMS ** -0.5, 0.09375, ((0, 16), (2, 16)))
    prior_var = draw_prior_var(jax.random.fold_in(key_list[4], 71), 0)
    return dict(probes=probes, map_real=map_real, map_imag=map_imag, prior_var=prior_var)


noise_ratio = 0.5

def reference(probes, map_real, map_imag, prior_var):
    time_steps = jnp.arange(STEPS, dtype=jnp.int32)
    bin_index = jnp.arange(BINS, dtype=jnp.int32)
    product_index = time_steps[:, None] * bin_index[None, :] % PERIOD
    angles = product_index.astype(jnp.float32) * (2.0 * jnp.pi / PERIOD)
    norm_scale = 1.0 / jnp.sqrt(jnp.float32(PERIOD))
    cosines = jnp.cos(angles) * norm_scale
    sines = jnp.sin(angles) * norm_scale
    bin_weight = jnp.where(bin_index == 0, 1.0, 2.0).astype(jnp.float32)
    flattened = probes.astype(jnp.float32).reshape(PROBES * SENSORS, STEPS)
    spec_real = jnp.dot(flattened, cosines, precision=lax.Precision.HIGHEST)
    spec_imag = -jnp.dot(flattened, sines, precision=lax.Precision.HIGHEST)
    spec_real = spec_real.astype(jnp.bfloat16).reshape(PROBES, SENSORS, BINS).transpose(2, 1, 0)
    spec_imag = spec_imag.astype(jnp.bfloat16).reshape(PROBES, SENSORS, BINS).transpose(2, 1, 0)
    spectra = jnp.concatenate([spec_real, spec_imag], axis=-1)

    def per_bin(items):
        real_block, imag_block, spec_block, weight_one = items
        left_real = jnp.dot(real_block.T, spec_block, preferred_element_type=jnp.float32)
        left_imag = jnp.dot(imag_block.T, spec_block, preferred_element_type=jnp.float32)
        u_real = left_real[:, :PROBES] + left_imag[:, PROBES:]
        u_imag = left_real[:, PROBES:] - left_imag[:, :PROBES]
        quadratic = weight_one * jnp.sum(prior_var[:, None] * (u_real * u_real + u_imag * u_imag))
        scaled = (jnp.concatenate([u_real, u_imag], axis=-1) * prior_var[:, None]).astype(jnp.bfloat16)
        right_real = jnp.dot(real_block, scaled, preferred_element_type=jnp.float32)
        right_imag = jnp.dot(imag_block, scaled, preferred_element_type=jnp.float32)
        w_real = right_real[:, :PROBES] - right_imag[:, PROBES:]
        w_imag = right_real[:, PROBES:] + right_imag[:, :PROBES]
        return (jnp.concatenate([w_real, w_imag], axis=-1).astype(jnp.bfloat16), quadratic)
    responses, quadratics = lax.map(per_bin, (map_real, map_imag, spectra, bin_weight))
    trace_est = jnp.sum(quadratics) / (PROBES * SENSORS * STEPS)
    responses = responses.astype(jnp.float32)
    w_real = responses[:, :, :PROBES].transpose(2, 1, 0).reshape(PROBES * SENSORS, BINS)
    w_imag = responses[:, :, PROBES:].transpose(2, 1, 0).reshape(PROBES * SENSORS, BINS)
    cos_weighted = (cosines * bin_weight[None, :]).T
    sin_weighted = (sines * bin_weight[None, :]).T
    response = jnp.dot(w_real, cos_weighted, precision=lax.Precision.HIGHEST) - jnp.dot(w_imag, sin_weighted, precision=lax.Precision.HIGHEST)
    response = response.reshape(PROBES, SENSORS, STEPS)
    return (response + noise_ratio * trace_est * probes.astype(jnp.float32)).astype(jnp.bfloat16)
```

```python
import functools

import jax
import jax.numpy as jnp
import numpy as np
from jax import lax
from jax.experimental import pallas as pl
from jax.experimental.pallas import tpu as pltpu
from jax.sharding import Mesh
from jax.sharding import PartitionSpec as P

SENSORS = 600
STEPS = 420
PERIOD = 840
PROBES = 64
BINS = 224
FREQ = ("zl", "y")
PAR = ("x", "h", "c")
BLOCKS = 16
BIN_DEV = BINS // BLOCKS
BIN_PAD = 16
ROWS = BLOCKS * BIN_PAD
XS = 4
NOISE = 0.5
TRACE_ROW = BIN_DEV
HALF = 208
SPAN = 216
UNROLL = 7

f32 = jnp.float32
bf16 = jnp.bfloat16
VMEM = pl.BlockSpec(memory_space=pltpu.VMEM)


def two_parts(values):
    values = values.astype(np.float32)
    upper = values.astype(bf16)
    return upper, (values - upper.astype(np.float32)).astype(bf16)


def tables():
    bins = np.arange(BINS)
    turn = (np.arange(STEPS)[:, None] * bins[None, :]) % PERIOD
    angle = turn * (2.0 * np.pi / PERIOD)
    both = np.stack([np.cos(angle), -np.sin(angle)]) / np.sqrt(float(PERIOD))
    both = both * np.where(bins == 0, 1.0, 2.0)
    both = both.reshape(2, STEPS, BLOCKS, BIN_DEV)
    both = np.pad(both, ((0, 0), (0, HALF + SPAN - STEPS), (0, 0), (0, BIN_PAD - BIN_DEV)))
    return np.stack(two_parts(both.reshape(2, HALF + SPAN, ROWS)), axis=1)


def dft_kernel(table, probes, out):
    probe = probes[lax.axis_index("x")]
    c = lax.axis_index("c")
    tn = (((0,), (0,)), ((), ()))
    d = sum(
        lax.dot_general(table[c, piece, :STEPS], probe, tn, preferred_element_type=f32)
        for piece in range(2)
    )
    row = lax.broadcasted_iota(jnp.int32, (ROWS, 1), 0)
    out[...] = (d * jnp.where(row == 0, 1.0, 0.5)).astype(bf16)


def middle_kernel(*refs):
    own, oth = refs[:XS], refs[XS : 2 * XS]
    map_real, map_imag, prior = refs[2 * XS : 2 * XS + 3]
    outs = refs[2 * XS + 3 :]
    w_own, w_oth, trace, scaled = outs[:XS], outs[XS : 2 * XS], outs[2 * XS], outs[2 * XS + 1]
    sigma = jnp.where(lax.axis_index("c") == 0, 1.0, -1.0).astype(f32)
    first = lax.axis_index(FREQ) == 0
    half = XS * BLOCKS
    nt = (((1,), (1,)), ((), ()))
    p = prior[...]

    def left(k):
        weight = jnp.where(first & (k == 0), 1.0, 2.0).astype(f32)
        v = jnp.concatenate([r[k] for r in own] + [r[k] for r in oth], axis=0)
        ar = jnp.dot(v, map_real[k], preferred_element_type=f32)
        ai = jnp.dot(v, map_imag[k], preferred_element_type=f32)
        u_own = ar[:half] + sigma * ai[half:]
        u_oth = ar[half:] - sigma * ai[:half]
        scaled[k, :half] = (u_own * p).astype(bf16)
        scaled[k, half:] = (u_oth * p).astype(bf16)
        return weight * p * jnp.sum(u_own * u_own + u_oth * u_oth, axis=0, keepdims=True)

    def right(k):
        a = scaled[k]
        br = lax.dot_general(a, map_real[k], nt, preferred_element_type=f32)
        bi = lax.dot_general(a, map_imag[k], nt, preferred_element_type=f32)
        to_own = (br[:half] - sigma * bi[half:]).astype(bf16)
        to_oth = (br[half:] + sigma * bi[:half]).astype(bf16)
        for j in range(XS):
            rows = slice(j * BLOCKS, (j + 1) * BLOCKS)
            w_own[j][k] = to_own[rows]
            w_oth[j][k] = to_oth[rows]

    def lefts(i, total):
        return total + sum(left(UNROLL * i + n) for n in range(UNROLL))

    def rights(i, _):
        for n in range(UNROLL):
            right(UNROLL * i + n)
        return 0

    trace[...] = lax.fori_loop(0, BIN_DEV // UNROLL, lefts, jnp.zeros(p.shape, f32))
    lax.fori_loop(0, BIN_DEV // UNROLL, rights, 0)


def trace_line(total):
    lane = lax.broadcasted_iota(jnp.int32, (1, SENSORS), 1)
    whole = jnp.full((1, SENSORS), total, f32)
    upper = whole.astype(bf16).astype(f32)
    return jnp.where(lane == 0, upper, jnp.where(lane == 1, whole - upper, 0.0)).astype(bf16)


def read_trace(ref, row):
    line = ref[row : row + 1, 0:2].astype(f32)
    return line[0, 0] + line[0, 1]


def inverse_kernel(table, own, oth, out):
    c = lax.axis_index("c")
    row = lax.broadcasted_iota(jnp.int32, (ROWS, 128), 0)
    lane = lax.broadcasted_iota(jnp.int32, (ROWS, 128), 1)
    marked = (row % BIN_PAD == TRACE_ROW) & (lane < 2)
    span = pl.ds(pl.multiple_of(c * HALF, 16), SPAN)
    total = jnp.zeros((), f32)
    r = jnp.zeros((SPAN, SENSORS), f32)
    for ref, part in ((own, c), (oth, 1 - c)):
        v = ref[0].astype(f32) + ref[1].astype(f32)
        total = total + jnp.sum(jnp.where(marked, v[:, :128], 0.0))
        v = v.astype(bf16)
        for piece in range(2):
            r = r + jnp.dot(table[part, piece, span], v, preferred_element_type=f32)
    out[...] = r.astype(bf16)
    out[SPAN - 1 : SPAN, :] = trace_line(total)


def finish_kernel(*refs):
    own, oth = refs[:XS], refs[XS : 2 * XS]
    probes, out = refs[2 * XS :]
    x, c = lax.axis_index("x"), lax.axis_index("c")
    total = sum(read_trace(r, SPAN - 1) for r in own)
    trace = total * (NOISE / (PROBES * SENSORS * STEPS))
    for j in range(XS):
        p = lax.rem(x + j, XS)
        for ref, half in ((own[j], c), (oth[j], 1 - c)):
            rows = pl.ds(pl.multiple_of(half * HALF, 16), HALF)
            out[p, rows, :] = (ref[0:HALF].astype(f32) + trace * probes[p, rows, :].astype(f32)).astype(bf16)
        rest = STEPS - 2 * HALF
        last = jnp.where(c == 1, own[j][HALF : HALF + rest].astype(f32), oth[j][HALF : HALF + rest].astype(f32))
        out[p, 2 * HALF :, :] = (last + trace * probes[p, 2 * HALF :, :].astype(f32)).astype(bf16)


def shift(value, axis, by):
    n = lax.axis_size(axis)
    return lax.ppermute(value, axis, [(i, (i + by) % n) for i in range(n)])


def swap_core(value):
    return lax.ppermute(value, "c", [(0, 1), (1, 0)])


def call(kernel, name, operands, outs, limit, scratch=()):
    return pl.pallas_call(
        kernel,
        in_specs=[VMEM] * len(operands),
        out_specs=[VMEM] * len(outs),
        out_shape=[jax.ShapeDtypeStruct(*o) for o in outs],
        scratch_shapes=list(scratch),
        name=name,
        compiler_params=pltpu.CompilerParams(vmem_limit_bytes=limit << 20),
    )(*operands)


def shards(probes, map_real, map_imag, prior_var):
    table = jnp.asarray(tables())
    by_time, probes = lax.optimization_barrier((probes.transpose(0, 2, 1), probes))
    (spectra,) = call(dft_kernel, "dft", (table, by_time), [((ROWS, SENSORS), bf16)], 4)
    arrived = lax.all_to_all(spectra.reshape(BLOCKS, BIN_PAD, SENSORS), FREQ, 0, 0, tiled=True)
    arrived = arrived.transpose(1, 0, 2)[:BIN_DEV]
    away = {j: shift(arrived, "x", -j) for j in (2, 1, 3)}
    own = [arrived] + [away[j] for j in range(1, XS)]
    other = [swap_core(v) for v in own]

    prior = prior_var[None, :]
    block = ((BIN_DEV, BLOCKS, SENSORS), bf16)
    *w, trace = call(
        middle_kernel,
        "middle",
        [*own, *other, map_real, map_imag, prior],
        [block] * (2 * XS) + [(prior.shape, f32)],
        4,
        [pltpu.VMEM((BIN_DEV, 2 * XS * BLOCKS, prior.shape[1]), bf16)],
    )
    both = {j: (w[j].astype(f32) + swap_core(w[XS + j]).astype(f32)).astype(bf16) for j in (2, 1, 3, 0)}
    total = both[0].astype(f32)
    for j in (2, 1, 3):
        total = total + shift(both[j], "x", j).astype(f32)
    total = total.astype(bf16).transpose(1, 0, 2)
    quad = jnp.sum(trace)
    quad_up = quad.astype(bf16)
    quad_low = (quad - quad_up.astype(f32)).astype(bf16)
    lane = jnp.arange(SENSORS)
    line = jnp.where(lane == 0, quad_up, jnp.where(lane == 1, quad_low, jnp.zeros((), bf16)))
    extra = jnp.where(
        jnp.arange(BIN_PAD - BIN_DEV)[None, :, None] == 0, line[None, None, :], jnp.zeros((), bf16)
    )
    extra = jnp.broadcast_to(extra, (BLOCKS, BIN_PAD - BIN_DEV, SENSORS))
    outgoing = jnp.concatenate([total, extra], axis=1)
    outgoing = jnp.broadcast_to(outgoing[None], (2, BLOCKS, BIN_PAD, SENSORS))
    outgoing = outgoing.reshape(2 * BLOCKS, BIN_PAD, SENSORS)
    arrived = lax.all_to_all(outgoing, ("h",) + FREQ, 0, 0, tiled=True)
    pieces = [v.reshape(2, ROWS, SENSORS) for v in (arrived, swap_core(arrived))]
    (part,) = call(inverse_kernel, "inverse", (table, *pieces), [((SPAN, SENSORS), bf16)], 4)
    away = {j: shift(part, "x", -j) for j in (2, 1, 3)}
    own = [part] + [away[j] for j in range(1, XS)]
    other = [swap_core(v) for v in own]
    (out,) = call(finish_kernel, "finish", (*own, *other, probes.transpose(0, 2, 1)), [((XS, STEPS, SENSORS), bf16)], 4)
    return out.transpose(0, 2, 1)


def solution(mesh):
    torus = Mesh(mesh.devices.reshape(4, 2, 2, 4, 4), ("x", "h", "c", "zl", "y"))
    in_specs = (P(FREQ, None, None), P(FREQ, None, PAR), P(FREQ, None, PAR), P(PAR))
    return jax.shard_map(
        shards, mesh=torus, in_specs=in_specs, out_specs=P(FREQ, None, None), check_vma=False
    )
```

```python
import functools

import jax
import jax.numpy as jnp
import numpy as np
from jax import lax
from jax.experimental import pallas as pl
from jax.experimental.pallas import tpu as pltpu
from jax.sharding import Mesh
from jax.sharding import PartitionSpec as P

SENSORS = 600
STEPS = 420
PERIOD = 840
PROBES = 64
BINS = 224
FREQ = ("zl", "y")
PAR = ("x", "h", "c")
BLOCKS = 16
BIN_DEV = BINS // BLOCKS
BIN_PAD = 16
ROWS = BLOCKS * BIN_PAD
XS = 4
NOISE = 0.5
TRACE_ROW = BIN_DEV
HALF = 208
SPAN = 216
HALF_BINS = BIN_DEV // 2
FLOPS = 2_000_000_000


f32 = jnp.float32
bf16 = jnp.bfloat16
VMEM = pl.BlockSpec(memory_space=pltpu.VMEM)


def two_parts(values):
    values = values.astype(np.float32)
    upper = values.astype(bf16)
    return upper, (values - upper.astype(np.float32)).astype(bf16)


def tables():
    bins = np.arange(BINS)
    turn = (np.arange(STEPS)[:, None] * bins[None, :]) % PERIOD
    angle = turn * (2.0 * np.pi / PERIOD)
    both = np.stack([np.cos(angle), -np.sin(angle)]) / np.sqrt(float(PERIOD))
    both = both * np.where(bins == 0, 1.0, 2.0)
    both = both.reshape(2, STEPS, BLOCKS, BIN_DEV)
    both = np.pad(both, ((0, 0), (0, HALF + SPAN - STEPS), (0, 0), (0, BIN_PAD - BIN_DEV)))
    return np.stack(two_parts(both.reshape(2, HALF + SPAN, ROWS)), axis=1)


def dft_kernel(table, probes, out):
    probe = probes[lax.axis_index("x")]
    c = lax.axis_index("c")
    tn = (((0,), (0,)), ((), ()))
    d = sum(
        lax.dot_general(table[c, piece, :STEPS], probe, tn, preferred_element_type=f32)
        for piece in range(2)
    )
    row = lax.broadcasted_iota(jnp.int32, (ROWS, 1), 0)
    out[...] = (d * jnp.where(row == 0, 1.0, 0.5)).astype(bf16)


def middle_kernel(base, *refs):
    own, oth = refs[:XS], refs[XS : 2 * XS]
    map_real, map_imag, prior = refs[2 * XS : 2 * XS + 3]
    before = refs[2 * XS + 3] if base else None
    w_own, w_oth, trace, scaled = refs[2 * XS + 3 + (base > 0) :]
    sigma = jnp.where(lax.axis_index("c") == 0, 1.0, -1.0).astype(f32)
    first = lax.axis_index(FREQ) == 0
    half = XS * BLOCKS
    nt = (((1,), (1,)), ((), ()))
    p = prior[...]

    def left(k):
        weight = jnp.where(first, 1.0, 2.0).astype(f32) if base + k == 0 else 2.0
        v = jnp.concatenate([own[j][k] for j in range(XS)] + [oth[0][base + k]] + [oth[j][k] for j in range(1, XS)], axis=0)
        ar = jnp.dot(v, map_real[base + k], preferred_element_type=f32)
        ai = jnp.dot(v, map_imag[base + k], preferred_element_type=f32)
        u_own = ar[:half] + sigma * ai[half:]
        u_oth = ar[half:] - sigma * ai[:half]
        scaled[k, :half] = (u_own * p).astype(bf16)
        scaled[k, half:] = (u_oth * p).astype(bf16)
        return weight * p * jnp.sum(u_own * u_own + u_oth * u_oth, axis=0, keepdims=True)

    def right(k):
        a = scaled[k]
        br = lax.dot_general(a, map_real[base + k], nt, preferred_element_type=f32)
        bi = lax.dot_general(a, map_imag[base + k], nt, preferred_element_type=f32)
        to_own = (br[:half] - sigma * bi[half:]).astype(bf16)
        to_oth = (br[half:] + sigma * bi[:half]).astype(bf16)
        for j in range(XS):
            rows = slice(j * BLOCKS, (j + 1) * BLOCKS)
            w_own[j, k] = to_own[rows]
            w_oth[j, k] = to_oth[rows]

    quad = sum(left(k) for k in range(HALF_BINS))
    for k in range(HALF_BINS):
        right(k)
    if base:
        trace[...] = trace_line(jnp.sum(quad + before[...]))
    else:
        trace[...] = quad


def trace_line(total):
    lane = lax.broadcasted_iota(jnp.int32, (1, SENSORS), 1)
    whole = jnp.full((1, SENSORS), total, f32)
    upper = whole.astype(bf16).astype(f32)
    return jnp.where(lane == 0, upper, jnp.where(lane == 1, whole - upper, 0.0)).astype(bf16)


def read_trace(ref, row):
    line = ref[row : row + 1, 0:2].astype(f32)
    return line[0, 0] + line[0, 1]


def inverse_kernel(table, own, oth, out):
    c = lax.axis_index("c")
    row = lax.broadcasted_iota(jnp.int32, (ROWS, 128), 0)
    lane = lax.broadcasted_iota(jnp.int32, (ROWS, 128), 1)
    marked = (row % BIN_PAD == TRACE_ROW) & (lane < 2)
    span = pl.ds(pl.multiple_of(c * HALF, 16), SPAN)
    total = jnp.zeros((), f32)
    r = jnp.zeros((SPAN, SENSORS), f32)
    for ref, part in ((own, c), (oth, 1 - c)):
        v = ref[0].astype(f32) + ref[1].astype(f32)
        total = total + jnp.sum(jnp.where(marked, v[:, :128], 0.0))
        v = v.astype(bf16)
        for piece in range(2):
            r = r + jnp.dot(table[part, piece, span], v, preferred_element_type=f32)
    out[...] = r.astype(bf16)
    out[SPAN - 1 : SPAN, :] = trace_line(total)


def finish_kernel(*refs):
    own, oth = refs[:XS], refs[XS : 2 * XS]
    probes, out = refs[2 * XS :]
    x, c = lax.axis_index("x"), lax.axis_index("c")
    total = sum(read_trace(r, SPAN - 1) for r in own)
    trace = total * (NOISE / (PROBES * SENSORS * STEPS))
    for j in range(XS):
        p = lax.rem(x + j, XS)
        for ref, half in ((own[j], c), (oth[j], 1 - c)):
            rows = pl.ds(pl.multiple_of(half * HALF, 16), HALF)
            out[p, rows, :] = (ref[0:HALF].astype(f32) + trace * probes[p, rows, :].astype(f32)).astype(bf16)
        rest = STEPS - 2 * HALF
        last = jnp.where(c == 1, own[j][HALF : HALF + rest].astype(f32), oth[j][HALF : HALF + rest].astype(f32))
        out[p, 2 * HALF :, :] = (last + trace * probes[p, 2 * HALF :, :].astype(f32)).astype(bf16)


def shift(value, axis, by):
    n = lax.axis_size(axis)
    return lax.ppermute(value, axis, [(i, (i + by) % n) for i in range(n)])


def swap_core(value):
    return lax.ppermute(value, "c", [(0, 1), (1, 0)])


def call(kernel, operands, outs, limit, scratch=(), flops=0):
    return pl.pallas_call(
        kernel,
        in_specs=[VMEM] * len(operands),
        out_specs=[VMEM] * len(outs),
        out_shape=[jax.ShapeDtypeStruct(*o) for o in outs],
        scratch_shapes=list(scratch),
        cost_estimate=pl.CostEstimate(flops=flops, bytes_accessed=0, transcendentals=0) if flops else None,
        compiler_params=pltpu.CompilerParams(vmem_limit_bytes=limit << 20),
    )(*operands)


def steps(probes, map_real, map_imag, prior_var):
    table = jnp.asarray(tables())
    by_time, probes = lax.optimization_barrier((probes.transpose(0, 2, 1), probes))
    (spectra,) = call(dft_kernel, (table, by_time), [((ROWS, SENSORS), bf16)], 4)
    arrived = lax.all_to_all(spectra.reshape(BLOCKS, BIN_PAD, SENSORS), FREQ, 0, 0, tiled=True)
    arrived = arrived.transpose(1, 0, 2)[:BIN_DEV]
    parts = [arrived[:HALF_BINS], arrived[HALF_BINS:]]
    away = [{j: shift(part, "x", -j) for j in (2, 1, 3)} for part in parts]
    own_other = swap_core(arrived)

    prior = prior_var[None, :]
    block = ((XS, HALF_BINS, BLOCKS, SENSORS), bf16)
    trace = None
    totals = []
    for at, part in enumerate(parts):
        near = [away[at][j] for j in range(1, XS)]
        w_own, w_oth, trace = call(
            functools.partial(middle_kernel, at * HALF_BINS),
            [part, *near, own_other, *[swap_core(v) for v in near], map_real, map_imag, prior]
            + ([] if trace is None else [trace]),
            [block] * 2 + [((1, SENSORS), bf16) if at else (prior.shape, f32)],
            4,
            [pltpu.VMEM((HALF_BINS, 2 * XS * BLOCKS, prior.shape[1]), bf16)],
            FLOPS,
        )
        from_core = swap_core(w_oth)
        both = [(w_own[j].astype(f32) + from_core[j].astype(f32)).astype(bf16) for j in range(XS)]
        total = both[0].astype(f32)
        for j in (2, 1, 3):
            total = total + shift(both[j], "x", j).astype(f32)
        totals.append(total.astype(bf16))
    extra = jnp.concatenate([trace, jnp.zeros_like(trace)])[:, None, :]
    extra = jnp.broadcast_to(extra, (BIN_PAD - BIN_DEV, BLOCKS, SENSORS))
    outgoing = jnp.concatenate([*totals, extra]).transpose(1, 0, 2)
    outgoing = jnp.broadcast_to(outgoing[None], (2, BLOCKS, BIN_PAD, SENSORS))
    outgoing = outgoing.reshape(2 * BLOCKS, BIN_PAD, SENSORS)
    arrived = lax.all_to_all(outgoing, ("h",) + FREQ, 0, 0, tiled=True)
    pieces = [v.reshape(2, ROWS, SENSORS) for v in (arrived, swap_core(arrived))]
    (part,) = call(inverse_kernel, (table, *pieces), [((SPAN, SENSORS), bf16)], 4)
    away = {j: shift(part, "x", -j) for j in (2, 1, 3)}
    own = [part] + [away[j] for j in range(1, XS)]
    other = [swap_core(v) for v in own]
    (out,) = call(finish_kernel, (*own, *other, probes.transpose(0, 2, 1)), [((XS, STEPS, SENSORS), bf16)], 4)
    return out.transpose(0, 2, 1)


def solution(mesh):
    torus = Mesh(mesh.devices.reshape(4, 2, 2, 4, 4), ("x", "h", "c", "zl", "y"))
    in_specs = (P(FREQ, None, None), P(FREQ, None, PAR), P(FREQ, None, PAR), P(PAR))
    return jax.shard_map(steps, mesh=torus, in_specs=in_specs, out_specs=P(FREQ, None, None), check_vma=False)
```

```python
import functools

import jax
import jax.numpy as jnp
import numpy as np
from jax import lax
from jax.experimental import pallas as pl
from jax.experimental.pallas import tpu as pltpu
from jax.experimental.layout import Layout, with_layout_constraint
from jax.sharding import Mesh
from jax.sharding import PartitionSpec as P

SENSORS = 600
STEPS = 420
PERIOD = 840
PROBES = 64
BINS = 224
FREQ = ("zl", "y")
PAR = ("x", "h", "c")
BLOCKS = 16
BIN_DEV = BINS // BLOCKS
BIN_PAD = 16
ROWS = BLOCKS * BIN_PAD
XS = 4
NOISE = 0.5
TRACE_ROW = BIN_DEV
HALF = 208
SPAN = 216
SPLIT = (112, 104)
HALF_BINS = BIN_DEV // 2
FLOPS = 2_000_000_000


f32 = jnp.float32
bf16 = jnp.bfloat16
VMEM = pl.BlockSpec(memory_space=pltpu.VMEM)


def tables():
    bins = np.arange(BINS)
    turn = (np.arange(STEPS)[:, None] * bins[None, :]) % PERIOD
    angle = turn * (2.0 * np.pi / PERIOD)
    both = np.stack([np.cos(angle), -np.sin(angle)]) / np.sqrt(float(PERIOD))
    both = both * np.where(bins == 0, 1.0, 2.0)
    both = both.reshape(2, STEPS, BLOCKS, BIN_DEV)
    both = np.pad(both, ((0, 0), (0, HALF + SPAN - STEPS), (0, 0), (0, BIN_PAD - BIN_DEV)))
    return both.reshape(2, HALF + SPAN, ROWS).astype(bf16)


def dft_kernel(table, probes, out):
    probe = probes[lax.axis_index("x")]
    c = lax.axis_index("c")
    tn = (((0,), (0,)), ((), ()))
    d = lax.dot_general(table[c, :STEPS], probe, tn, preferred_element_type=f32)
    row = lax.broadcasted_iota(jnp.int32, (ROWS, 1), 0)
    out[...] = (d * jnp.where(row == 0, 1.0, 0.5)).astype(bf16)


def middle_kernel(base, *refs):
    own, oth = refs[:XS], refs[XS : 2 * XS]
    map_real, map_imag, prior = refs[2 * XS : 2 * XS + 3]
    before = refs[2 * XS + 3] if base else None
    w_own, w_oth, trace, scaled = refs[2 * XS + 3 + (base > 0) :]
    sigma = jnp.where(lax.axis_index("c") == 0, 1.0, -1.0).astype(f32)
    first = lax.axis_index(FREQ) == 0
    half = XS * BLOCKS
    nt = (((1,), (1,)), ((), ()))
    p = prior[...]

    def left(k):
        weight = jnp.where(first, 1.0, 2.0).astype(f32) if base + k == 0 else 2.0
        v = jnp.concatenate([own[j][k] for j in range(XS)] + [oth[0][base + k]] + [oth[j][k] for j in range(1, XS)], axis=0)
        ar = jnp.dot(v, map_real[base + k], preferred_element_type=f32)
        ai = jnp.dot(v, map_imag[base + k], preferred_element_type=f32)
        u_own = ar[:half] + sigma * ai[half:]
        u_oth = ar[half:] - sigma * ai[:half]
        scaled[k, :half] = (u_own * p).astype(bf16)
        scaled[k, half:] = (u_oth * p).astype(bf16)
        return weight * p * jnp.sum(u_own * u_own + u_oth * u_oth, axis=0, keepdims=True)

    def right(k):
        a = scaled[k]
        br = lax.dot_general(a, map_real[base + k], nt, preferred_element_type=f32)
        bi = lax.dot_general(a, map_imag[base + k], nt, preferred_element_type=f32)
        to_own = (br[:half] - sigma * bi[half:]).astype(bf16)
        to_oth = (br[half:] + sigma * bi[:half]).astype(bf16)
        for j in range(XS):
            rows = slice(j * BLOCKS, (j + 1) * BLOCKS)
            w_own[j, k] = to_own[rows]
            w_oth[j, k] = to_oth[rows]

    quad = sum(left(k) for k in range(HALF_BINS))
    for k in range(HALF_BINS):
        right(k)
    if base:
        trace[...] = trace_line(jnp.sum(quad + before[...]))
    else:
        trace[...] = quad


def trace_line(total):
    lane = lax.broadcasted_iota(jnp.int32, (1, SENSORS), 1)
    whole = jnp.full((1, SENSORS), total, f32)
    upper = whole.astype(bf16).astype(f32)
    return jnp.where(lane == 0, upper, jnp.where(lane == 1, whole - upper, 0.0)).astype(bf16)


def read_trace(ref, row):
    line = ref[row : row + 1, 0:2].astype(f32)
    return line[0, 0] + line[0, 1]


def inverse_kernel(table, own, oth, early, late):
    c = lax.axis_index("c")
    row = lax.broadcasted_iota(jnp.int32, (ROWS, 128), 0)
    lane = lax.broadcasted_iota(jnp.int32, (ROWS, 128), 1)
    marked = (row % BIN_PAD == TRACE_ROW) & (lane < 2)
    span = pl.ds(pl.multiple_of(c * HALF, 16), SPAN)
    total = jnp.zeros((), f32)
    r = jnp.zeros((SPAN, SENSORS), f32)
    for ref, part in ((own, c), (oth, 1 - c)):
        v = ref[0].astype(f32) + ref[1].astype(f32)
        total = total + jnp.sum(jnp.where(marked, v[:, :128], 0.0))
        r = r + jnp.dot(table[part, span], v.astype(bf16), preferred_element_type=f32)
    early[...] = r[: SPLIT[0]].astype(bf16)
    late[...] = r[SPLIT[0] :].astype(bf16)
    late[SPLIT[1] - 1 :, :] = trace_line(total)


def assemble_kernel(*refs):
    own, oth = refs[: 2 * XS], refs[2 * XS : 4 * XS]
    out, noise = refs[4 * XS :]
    x, c = lax.axis_index("x"), lax.axis_index("c")
    total = sum(read_trace(r, SPLIT[1] - 1) for r in own[XS:])
    noise[...] = jnp.full(noise.shape, total * (NOISE / (PROBES * SENSORS * STEPS)), f32)
    rest = STEPS - 2 * HALF
    first, second = SPLIT[0], HALF - SPLIT[0]
    for j in range(XS):
        p = lax.rem(x + j, XS)
        for refs_of, half in ((own, c), (oth, 1 - c)):
            at = pl.multiple_of(half * HALF, 16)
            out[p, pl.ds(at, first), :] = refs_of[j][...]
            out[p, pl.ds(pl.multiple_of(at + first, 16), second), :] = refs_of[XS + j][:second]
        tail = slice(second, second + rest)
        out[p, 2 * HALF :, :] = jnp.where(c == 1, own[XS + j][tail], oth[XS + j][tail])


def shift(value, axis, by):
    n = lax.axis_size(axis)
    return lax.ppermute(value, axis, [(i, (i + by) % n) for i in range(n)])


def gather_ring(parts):
    a, b = parts
    a3 = shift(a, "x", 1)
    b1 = shift(b, "x", -1)
    b3 = shift(b, "x", 1)
    a1 = shift(a, "x", -1)
    a2 = shift(a3, "x", 1)
    b2 = shift(b1, "x", -1)
    return (a1, a2, a3), (b1, b2, b3)


def swap_core(value):
    return lax.ppermute(value, "c", [(0, 1), (1, 0)])


def call(kernel, operands, outs, limit, scratch=(), flops=0):
    return pl.pallas_call(
        kernel,
        in_specs=[VMEM] * len(operands),
        out_specs=[VMEM] * len(outs),
        out_shape=[jax.ShapeDtypeStruct(*o) for o in outs],
        scratch_shapes=list(scratch),
        cost_estimate=pl.CostEstimate(flops=flops, bytes_accessed=0, transcendentals=0) if flops else None,
        compiler_params=pltpu.CompilerParams(vmem_limit_bytes=limit << 20),
    )(*operands)


def steps(probes, map_real, map_imag, prior_var):
    table = jnp.asarray(tables())
    by_time, probes = lax.optimization_barrier((probes.transpose(0, 2, 1), probes))
    (spectra,) = call(dft_kernel, (table, by_time), [((ROWS, SENSORS), bf16)], 4)
    arrived = lax.all_to_all(spectra.reshape(BLOCKS, BIN_PAD, SENSORS), FREQ, 0, 0, tiled=True)
    arrived = arrived.transpose(1, 0, 2)[:BIN_DEV]
    parts = [arrived[:HALF_BINS], arrived[HALF_BINS:]]
    near = [[None] * (XS - 1) for _ in parts]
    for at, part in enumerate(parts):
        for j in (2, 1, 3):
            near[at][j - 1] = shift(part, "x", -j)
    own_other = swap_core(arrived)

    prior = prior_var[None, :]
    block = ((XS, HALF_BINS, BLOCKS, SENSORS), bf16)
    trace = None
    totals = []
    for at, part in enumerate(parts):
        w_own, w_oth, trace = call(
            functools.partial(middle_kernel, at * HALF_BINS),
            [part, *near[at], own_other, *[swap_core(v) for v in near[at]], map_real, map_imag, prior]
            + ([] if trace is None else [trace]),
            [block] * 2 + [((1, SENSORS), bf16) if at else (prior.shape, f32)],
            4,
            [pltpu.VMEM((HALF_BINS, 2 * XS * BLOCKS, prior.shape[1]), bf16)],
            FLOPS,
        )
        from_core = swap_core(w_oth)
        both = [(w_own[j].astype(f32) + from_core[j].astype(f32)).astype(bf16) for j in range(XS)]
        total = both[0].astype(f32)
        for j in (2, 1, 3):
            total = total + shift(both[j], "x", j).astype(f32)
        totals.append(total.astype(bf16))
    extra = jnp.concatenate([trace, jnp.zeros_like(trace)])[:, None, :]
    extra = jnp.broadcast_to(extra, (BIN_PAD - BIN_DEV, BLOCKS, SENSORS))
    outgoing = jnp.concatenate([*totals, extra]).transpose(1, 0, 2)
    outgoing = jnp.broadcast_to(outgoing[None], (2, BLOCKS, BIN_PAD, SENSORS))
    outgoing = outgoing.reshape(2 * BLOCKS, BIN_PAD, SENSORS)
    arrived = lax.all_to_all(outgoing, ("h",) + FREQ, 0, 0, tiled=True)
    pieces = [v.reshape(2, ROWS, SENSORS) for v in (arrived, swap_core(arrived))]
    parts = call(inverse_kernel, (table, *pieces), [((n, SENSORS), bf16) for n in SPLIT], 4)
    near = gather_ring(parts)
    own = [v for at in range(2) for v in (parts[at], *near[at])]
    other = [swap_core(v) for v in own]
    response, noise = call(assemble_kernel, (*own, *other), [((XS, STEPS, SENSORS), bf16), ((1, 128), f32)], 4)
    response = with_layout_constraint(response.transpose(0, 2, 1), Layout((2, 0, 1))).astype(f32)
    return (response + noise[0, 0] * probes.astype(f32)).astype(bf16)


def solution(mesh):
    torus = Mesh(mesh.devices.reshape(4, 2, 2, 4, 4), ("x", "h", "c", "zl", "y"))
    in_specs = (P(FREQ, None, None), P(FREQ, None, PAR), P(FREQ, None, PAR), P(PAR))
    return jax.shard_map(steps, mesh=torus, in_specs=in_specs, out_specs=P(FREQ, None, None), check_vma=False)
```

```python
import functools

import jax
import jax.numpy as jnp
import numpy as np
from jax import lax
from jax.experimental import pallas as pl
from jax.experimental.pallas import tpu as pltpu
from jax.experimental.layout import Layout, with_layout_constraint
from jax.sharding import Mesh
from jax.sharding import PartitionSpec as P

SENSORS = 600
STEPS = 420
PERIOD = 840
PROBES = 64
BINS = 224
FREQ = ("zl", "y")
PAR = ("x", "h", "c")
BLOCKS = 16
BIN_DEV = BINS // BLOCKS
BIN_PAD = 16
ROWS = BLOCKS * BIN_PAD
XS = 4
NOISE = 0.5
TRACE_ROW = BIN_DEV
HALF = 208
SPAN = 216
SPLIT = (112, 104)
HALF_BINS = BIN_DEV // 2
FLOPS = 2_000_000_000


f32 = jnp.float32
bf16 = jnp.bfloat16
VMEM = pl.BlockSpec(memory_space=pltpu.VMEM)


def tables():
    bins = np.arange(BINS)
    turn = (np.arange(STEPS)[:, None] * bins[None, :]) % PERIOD
    angle = turn * (2.0 * np.pi / PERIOD)
    both = np.stack([np.cos(angle), -np.sin(angle)]) / np.sqrt(float(PERIOD))
    both = both * np.where(bins == 0, 1.0, 2.0)
    both = both.reshape(2, STEPS, BLOCKS, BIN_DEV)
    both = np.pad(both, ((0, 0), (0, HALF + SPAN - STEPS), (0, 0), (0, BIN_PAD - BIN_DEV)))
    return both.reshape(2, HALF + SPAN, ROWS).astype(bf16)


def dft_kernel(table, probes, out):
    probe = probes[lax.axis_index("x")]
    c = lax.axis_index("c")
    tn = (((0,), (0,)), ((), ()))
    d = lax.dot_general(table[c, :STEPS], probe, tn, preferred_element_type=f32)
    row = lax.broadcasted_iota(jnp.int32, (ROWS, 1), 0)
    out[...] = (d * jnp.where(row == 0, 1.0, 0.5)).astype(bf16)


def middle_kernel(base, *refs):
    own, oth = refs[:XS], refs[XS : 2 * XS]
    map_real, map_imag, prior = refs[2 * XS : 2 * XS + 3]
    before = refs[2 * XS + 3] if base else None
    w_own, w_oth, trace, scaled = refs[2 * XS + 3 + (base > 0) :]
    sigma = jnp.where(lax.axis_index("c") == 0, 1.0, -1.0).astype(f32)
    first = lax.axis_index(FREQ) == 0
    half = XS * BLOCKS
    nt = (((1,), (1,)), ((), ()))
    p = prior[...]

    def left(k):
        weight = jnp.where(first, 1.0, 2.0).astype(f32) if base + k == 0 else 2.0
        v = jnp.concatenate([own[j][k] for j in range(XS)] + [oth[0][base + k]] + [oth[j][k] for j in range(1, XS)], axis=0)
        ar = jnp.dot(v, map_real[base + k], preferred_element_type=f32)
        ai = jnp.dot(v, map_imag[base + k], preferred_element_type=f32)
        u_own = ar[:half] + sigma * ai[half:]
        u_oth = ar[half:] - sigma * ai[:half]
        scaled[k, :half] = (u_own * p).astype(bf16)
        scaled[k, half:] = (u_oth * p).astype(bf16)
        return weight * p * jnp.sum(u_own * u_own + u_oth * u_oth, axis=0, keepdims=True)

    def right(k):
        a = scaled[k]
        br = lax.dot_general(a, map_real[base + k], nt, preferred_element_type=f32)
        bi = lax.dot_general(a, map_imag[base + k], nt, preferred_element_type=f32)
        to_own = (br[:half] - sigma * bi[half:]).astype(bf16)
        to_oth = (br[half:] + sigma * bi[:half]).astype(bf16)
        for j in range(XS):
            rows = slice(j * BLOCKS, (j + 1) * BLOCKS)
            w_own[j, k] = to_own[rows]
            w_oth[j, k] = to_oth[rows]

    quad = sum(left(k) for k in range(HALF_BINS))
    for k in range(HALF_BINS):
        right(k)
    if base:
        trace[...] = trace_line(jnp.sum(quad + before[...]))
    else:
        trace[...] = quad


def trace_line(total):
    lane = lax.broadcasted_iota(jnp.int32, (1, SENSORS), 1)
    whole = jnp.full((1, SENSORS), total, f32)
    upper = whole.astype(bf16).astype(f32)
    return jnp.where(lane == 0, upper, jnp.where(lane == 1, whole - upper, 0.0)).astype(bf16)


def read_trace(ref, row):
    line = ref[row : row + 1, 0:2].astype(f32)
    return line[0, 0] + line[0, 1]


def inverse_kernel(table, arrived, kept, sent):
    c = lax.axis_index("c")
    row = lax.broadcasted_iota(jnp.int32, (ROWS, 128), 0)
    lane = lax.broadcasted_iota(jnp.int32, (ROWS, 128), 1)
    v = arrived[0].astype(f32) + arrived[1].astype(f32)
    marked = (row % BIN_PAD == TRACE_ROW) & (lane < 2)
    total = jnp.sum(jnp.where(marked, v[:, :128], 0.0))
    v = v.astype(bf16)
    for half, out in ((1 - c, sent), (c, kept)):
        span = pl.ds(pl.multiple_of(half * HALF, 16), SPAN)
        out[...] = jnp.dot(table[c, span], v, preferred_element_type=f32).astype(out.dtype)
    sent[SPAN - 1 :, :] = trace_line(total)
    kept[SPAN - 1 :, :] = jnp.full((1, SENSORS), total, f32)


def join_kernel(kept, received, early, late):
    r = kept[...] + received[...].astype(f32)
    total = kept[SPAN - 1, 0] + read_trace(received, SPAN - 1)
    early[...] = r[: SPLIT[0]].astype(bf16)
    late[...] = r[SPLIT[0] :].astype(bf16)
    late[SPLIT[1] - 1 :, :] = trace_line(total)


def assemble_kernel(*refs):
    own, oth = refs[: 2 * XS], refs[2 * XS : 4 * XS]
    out, noise = refs[4 * XS :]
    x, c = lax.axis_index("x"), lax.axis_index("c")
    total = sum(read_trace(r, SPLIT[1] - 1) for r in own[XS:])
    noise[...] = jnp.full(noise.shape, total * (NOISE / (PROBES * SENSORS * STEPS)), f32)
    rest = STEPS - 2 * HALF
    first, second = SPLIT[0], HALF - SPLIT[0]
    for j in range(XS):
        p = lax.rem(x + j, XS)
        for refs_of, half in ((own, c), (oth, 1 - c)):
            at = pl.multiple_of(half * HALF, 16)
            out[p, pl.ds(at, first), :] = refs_of[j][...]
            out[p, pl.ds(pl.multiple_of(at + first, 16), second), :] = refs_of[XS + j][:second]
        tail = slice(second, second + rest)
        out[p, 2 * HALF :, :] = jnp.where(c == 1, own[XS + j][tail], oth[XS + j][tail])


def shift(value, axis, by):
    n = lax.axis_size(axis)
    return lax.ppermute(value, axis, [(i, (i + by) % n) for i in range(n)])


def gather_ring(parts):
    a, b = parts
    a3 = shift(a, "x", 1)
    b1 = shift(b, "x", -1)
    b3 = shift(b, "x", 1)
    a1 = shift(a, "x", -1)
    a2 = shift(a3, "x", 1)
    b2 = shift(b1, "x", -1)
    return (a1, a2, a3), (b1, b2, b3)


def swap_core(value):
    return lax.ppermute(value, "c", [(0, 1), (1, 0)])


def call(kernel, operands, outs, limit, scratch=(), flops=0):
    return pl.pallas_call(
        kernel,
        in_specs=[VMEM] * len(operands),
        out_specs=[VMEM] * len(outs),
        out_shape=[jax.ShapeDtypeStruct(*o) for o in outs],
        scratch_shapes=list(scratch),
        cost_estimate=pl.CostEstimate(flops=flops, bytes_accessed=0, transcendentals=0) if flops else None,
        compiler_params=pltpu.CompilerParams(vmem_limit_bytes=limit << 20),
    )(*operands)


def steps(probes, map_real, map_imag, prior_var):
    table = jnp.asarray(tables())
    by_time, probes = lax.optimization_barrier((probes.transpose(0, 2, 1), probes))
    (spectra,) = call(dft_kernel, (table, by_time), [((ROWS, SENSORS), bf16)], 4)
    arrived = lax.all_to_all(spectra.reshape(BLOCKS, BIN_PAD, SENSORS), FREQ, 0, 0, tiled=True)
    arrived = arrived.transpose(1, 0, 2)[:BIN_DEV]
    parts = [arrived[:HALF_BINS], arrived[HALF_BINS:]]
    near = [[None] * (XS - 1) for _ in parts]
    for at, part in enumerate(parts):
        for j in (2, 1, 3):
            near[at][j - 1] = shift(part, "x", -j)
    own_other = swap_core(arrived)

    prior = prior_var[None, :]
    block = ((XS, HALF_BINS, BLOCKS, SENSORS), bf16)
    trace = None
    totals = []
    for at, part in enumerate(parts):
        w_own, w_oth, trace = call(
            functools.partial(middle_kernel, at * HALF_BINS),
            [part, *near[at], own_other, *[swap_core(v) for v in near[at]], map_real, map_imag, prior]
            + ([] if trace is None else [trace]),
            [block] * 2 + [((1, SENSORS), bf16) if at else (prior.shape, f32)],
            4,
            [pltpu.VMEM((HALF_BINS, 2 * XS * BLOCKS, prior.shape[1]), bf16)],
            FLOPS,
        )
        from_core = swap_core(w_oth)
        both = [(w_own[j].astype(f32) + from_core[j].astype(f32)).astype(bf16) for j in range(XS)]
        total = both[0].astype(f32)
        for j in (2, 1, 3):
            total = total + shift(both[j], "x", j).astype(f32)
        totals.append(total.astype(bf16))
    extra = jnp.concatenate([trace, jnp.zeros_like(trace)])[:, None, :]
    extra = jnp.broadcast_to(extra, (BIN_PAD - BIN_DEV, BLOCKS, SENSORS))
    outgoing = jnp.concatenate([*totals, extra]).transpose(1, 0, 2)
    outgoing = jnp.broadcast_to(outgoing[None], (2, BLOCKS, BIN_PAD, SENSORS))
    outgoing = outgoing.reshape(2 * BLOCKS, BIN_PAD, SENSORS)
    arrived = lax.all_to_all(outgoing, ("h",) + FREQ, 0, 0, tiled=True)
    kept, sent = call(
        inverse_kernel, (table, arrived.reshape(2, ROWS, SENSORS)), [((SPAN, SENSORS), f32), ((SPAN, SENSORS), bf16)], 4
    )
    parts = call(join_kernel, (kept, swap_core(sent)), [((n, SENSORS), bf16) for n in SPLIT], 4)
    near = gather_ring(parts)
    own = [v for at in range(2) for v in (parts[at], *near[at])]
    other = [swap_core(v) for v in own]
    response, noise = call(assemble_kernel, (*own, *other), [((XS, STEPS, SENSORS), bf16), ((1, 128), f32)], 4)
    response = with_layout_constraint(response.transpose(0, 2, 1), Layout((2, 0, 1))).astype(f32)
    return (response + noise[0, 0] * probes.astype(f32)).astype(bf16)


def solution(mesh):
    torus = Mesh(mesh.devices.reshape(4, 2, 2, 4, 4), ("x", "h", "c", "zl", "y"))
    in_specs = (P(FREQ, None, None), P(FREQ, None, PAR), P(FREQ, None, PAR), P(PAR))
    return jax.shard_map(steps, mesh=torus, in_specs=in_specs, out_specs=P(FREQ, None, None), check_vma=False)
```
